32 devices in a mesh: seq: 8 (over y, x, core), head: 4 (over z).
Axes of the slice: x: 2, y: 2, z: 4, core: 2. Of those that a mesh axis runs over, the one named last changes fastest.
Arguments:
- video_rows: bfloat16 [4096, 5120], P('seq'), may hold values from -6 to 6
- context: bfloat16 [512, 5120], P('seq'), may hold values from -6 to 6
- valid_length: int32 [1], replicated, may hold values from 64 to 512
- timestep: int32 [1], replicated, may hold values from 0 to 999
- query_weight: bfloat16 [5120, 1024], P('seq', 'head'), may hold values from -0.078125 to 0.078125
- key_weight: bfloat16 [5120, 1024], P('seq', 'head'), may hold values from -0.078125 to 0.078125
- value_weight: bfloat16 [5120, 1024], P('seq', 'head'), may hold values from -0.078125 to 0.078125
- out_weight: bfloat16 [1024, 5120], P('head', 'seq'), may hold values from -0.1875 to 0.1875
- query_gain: float32 [1024], P('head'), may hold values from 0.5 to 15
- key_gain: float32 [1024], P('head'), may hold values from 0.5 to 15
- time_weight: bfloat16 [2, 256, 5120], P(None, None, 'head'), may hold values from -0.375 to 0.375
- modulation: float32 [2, 5120], P(None, 'head'), may hold values from -3 to 3
Outputs:
- residual_out: bfloat16 [4096, 5120], P('seq', 'head')
- modulated: bfloat16 [4096, 5120], P('seq', 'head')
The draws below stay inside these ranges and needn't reach their ends.
Inputs may be any that keep to these rules, and one draw needn't show every extreme that they name: `valid_length`: text positions at or beyond it are padding.
All inputs are finite; a program needn't handle non-finite values.
Results may differ from the reference program's by a relative error of at most 0.0065.
The reference program's roundings to bfloat16 on the way (of `normed`, `value_proj`, `query_normed`, `key_normed`, `weights`, `attended` and `act`) count: a program that leaves them out, or rounds other values in their place, can miss the bound.
Values may be sent and summed in bfloat16 or wider, within the bound.
A program may use at most 64 MiB of HBM per device.

```python
import jax
import jax.numpy as jnp
from jax import lax

D = 5120
HD = 128
TEXT = 512
FREQ = 256
HEADS = 8
ATT = 1024
TOKENS = 4096


def head_gains(key):
    base = jax.random.uniform(key, (HEADS, HD), jnp.float32, 0.5, 1.5)
    return base.reshape(HEADS * HD)


def draw_query_gain(key, part):
    return head_gains(jax.random.fold_in(key, 11))


def draw_key_gain(key, part):
    return head_gains(jax.random.fold_in(key, 23))


def shard_levels(rng, shape, cuts, least, top_value):
    def one(axis_at, parts):
        steps = jax.random.uniform(jax.random.fold_in(jax.random.fold_in(rng, 6), axis_at), (parts,), jnp.float32, least / len(cuts), top_value / len(cuts))
        return jnp.repeat(jnp.exp(steps), shape[axis_at] // parts).reshape((-1,) + (1,) * (len(shape) - axis_at - 1))

    loudness = one(*cuts[0])
    for cut in cuts[1:]:
        loudness = loudness * one(*cut)
    return loudness


def centred(own_key, shape, deviation, limit, pieces=(), held_as=jnp.bfloat16):
    loudness = shard_levels(own_key, shape, pieces, -0.22, 0.18) if pieces else 1.0
    entries = jax.random.normal(own_key, shape, jnp.float32) * deviation * loudness
    return jnp.minimum(jnp.maximum(entries, -limit), limit).astype(held_as)


def setup_inputs(seed: int = 0) -> dict:
    arg_keys = jax.random.split(jax.random.key(seed), 13)
    video_rows = centred(arg_keys[0], (TOKENS, D), 1.0, 6.0, ((0, 8),))
    context = centred(arg_keys[1], (TEXT, D), 1.0, 6.0, ((0, 8),))
    valid_length = jax.random.randint(arg_keys[2], (1,), TEXT // 8, TEXT + 1).astype(jnp.int32)
    timestep = jax.random.randint(arg_keys[3], (1,), 0, 1000).astype(jnp.int32)
    query_weight = centred(arg_keys[4], (D, ATT), D ** -0.5, 0.078125, ((0, 8), (1, 4)))
    key_weight = centred(arg_keys[5], (D, ATT), D ** -0.5, 0.078125, ((0, 8), (1, 4)))
    value_weight = centred(arg_keys[6], (D, ATT), D ** -0.5, 0.078125, ((0, 8), (1, 4)))
    out_weight = centred(arg_keys[7], (ATT, D), ATT ** -0.5, 0.1875, ((0, 4), (1, 8)))
    query_gain = draw_query_gain(jax.random.fold_in(arg_keys[12], 71), 0)
    key_gain = draw_key_gain(jax.random.fold_in(arg_keys[12], 71), 0)
    time_weight = centred(arg_keys[10], (2, FREQ, D), FREQ ** -0.5, 0.375, ((2, 4),))
    modulation = centred(arg_keys[11], (2, D), 0.5, 3.0, ((1, 4),), jnp.float32)
    return {"video_rows": video_rows, "context": context, "valid_length": valid_length, "timestep": timestep, "query_weight": query_weight, "key_weight": key_weight, "value_weight": value_weight, "out_weight": out_weight, "query_gain": query_gain, "key_gain": key_gain, "time_weight": time_weight, "modulation": modulation}


def layer_norm(rows):
    mean = lax.optimization_barrier(jnp.mean(rows, axis=-1, keepdims=True))
    spread = lax.optimization_barrier(jnp.mean((rows - mean) ** 2, axis=-1, keepdims=True))
    return (rows - mean) / jnp.sqrt(spread + 1e-06)

def rms_gain(rows, gain):
    return rows / jnp.sqrt(lax.optimization_barrier(jnp.mean(rows * rows, axis=-1, keepdims=True)) + 1e-06) * gain

def reference(video_rows, context, valid_length, timestep, query_weight, key_weight, value_weight, out_weight, query_gain, key_gain, time_weight, modulation):
    normed = layer_norm(video_rows.astype(jnp.float32)).astype(jnp.bfloat16)
    queries = jnp.dot(normed, query_weight, preferred_element_type=jnp.float32)
    key_proj = jnp.dot(context, key_weight, preferred_element_type=jnp.float32)
    value_proj = jnp.dot(context, value_weight, preferred_element_type=jnp.float32).astype(jnp.bfloat16)
    query_normed = rms_gain(queries, query_gain).astype(jnp.bfloat16)
    key_normed = rms_gain(key_proj, key_gain).astype(jnp.bfloat16)
    key_valid = jnp.arange(TEXT, dtype=jnp.int32) < valid_length[0]

    def one_head(head_index):
        offset = (head_index * HD).astype(jnp.int32)
        query_part = lax.dynamic_slice_in_dim(query_normed, offset, HD, 1)
        key_part = lax.dynamic_slice_in_dim(key_normed, offset, HD, 1)
        value_part = lax.dynamic_slice_in_dim(value_proj, offset, HD, 1)
        scores = jnp.dot(query_part, key_part.T, preferred_element_type=jnp.float32) * HD ** (-0.5)
        scores = jnp.where(key_valid[None, :], scores, jnp.float32(-1e+30))
        shifted = jnp.exp(scores - lax.optimization_barrier(jnp.max(scores, axis=-1, keepdims=True)))
        weights = (shifted / lax.optimization_barrier(jnp.sum(shifted, axis=-1, keepdims=True))).astype(jnp.bfloat16)
        return jnp.dot(weights, value_part, preferred_element_type=jnp.float32).astype(jnp.bfloat16)
    per_head = lax.map(one_head, jnp.arange(HEADS, dtype=jnp.int32))
    attended = jnp.transpose(per_head, (1, 0, 2)).reshape(TOKENS, ATT)
    projected = jnp.dot(attended, out_weight, preferred_element_type=jnp.float32)
    residual_out = (video_rows.astype(jnp.float32) + projected).astype(jnp.bfloat16)
    half = FREQ // 2
    freqs = jnp.exp(-jnp.log(10000.0) * jnp.arange(half, dtype=jnp.float32) / half)
    angles = timestep[0].astype(jnp.float32) * freqs
    embedding = jnp.concatenate([jnp.cos(angles), jnp.sin(angles)])
    act = jax.nn.silu(embedding).astype(jnp.bfloat16)[None, :]
    shift = modulation[0] + jnp.dot(act, time_weight[0], preferred_element_type=jnp.float32)[0]
    scale = modulation[1] + jnp.dot(act, time_weight[1], preferred_element_type=jnp.float32)[0]
    resid = residual_out.astype(jnp.float32)
    mean2 = lax.optimization_barrier(jnp.mean(resid, axis=-1, keepdims=True))
    var2 = lax.optimization_barrier(jnp.mean(resid * resid, axis=-1, keepdims=True)) - mean2 * mean2
    modulated = ((resid - mean2) / jnp.sqrt(var2 + 1e-06) * (1.0 + scale) + shift).astype(jnp.bfloat16)
    return (residual_out, modulated)
```

```python
import functools

import jax
import jax.numpy as jnp
from jax import lax
from jax.experimental import pallas as pl
from jax.experimental.pallas import tpu as pltpu
from jax.sharding import PartitionSpec as P

HD = 128
FREQ = 256
LANES = 128
F32 = jnp.float32
BF16 = jnp.bfloat16
MESH_ID = pl.DeviceIdType.MESH


def flip(index, mask):
    bit = 1
    while bit <= mask:
        if mask & bit:
            index = index + bit - 2 * bit * ((index // bit) % 2)
        bit *= 2
    return index


def rows_to_lanes(column, tall):
    return jnp.transpose(jnp.broadcast_to(column, (tall, LANES)))[:8]


def body(
    n_seq, n_head, chunks,
    valid, video, ctx, qw, kw, vw, ow, qg, kg, act, tw, mod, vpart,
    resid_out, mod_out,
    vid, normed, ctxg, qwg, part, pair, rsg, own_kv, kvg, spread, owg, attg,
    queries, qsq, ksq, stat, shsc,
    vid_sem, loc_sem, ctx_s, ctx_r, qw_s, qw_r, pr_s, pr_r, rs_s, rs_r, kv_s, kv_r,
    sp_s, sp_r, oz_s, oz_r, og_s, og_r, ksq_s, ksq_r, qsq_s, qsq_r, at_s, at_r, st_s, st_r,
):
    s = lax.axis_index("seq")
    z = lax.axis_index("head")
    core = s % 2
    chip = s // 2
    n_chip = n_seq // 2
    ratio = n_seq // n_head
    tok, width = vid.shape
    depth = qw.shape[0]
    att = qw.shape[1]
    text = ctx.shape[-2]
    sent = []

    def to_seq(k):
        return (flip(s, k), z)

    def to_head(k):
        return (s, flip(z, k))

    def remote(src, dst, ssem, rsem, dev):
        return pltpu.make_async_remote_copy(
            src_ref=src, dst_ref=dst, send_sem=ssem, recv_sem=rsem,
            device_id=dev, device_id_type=MESH_ID,
        )

    def push(src, dst, ssem, rsem, dev):
        copy = remote(src, dst, ssem, rsem, dev)
        copy.start()
        sent.append(copy)

    def arrived(dst, ssem, rsem, dev):
        remote(dst, dst, ssem, rsem, dev).wait_recv()

    def gather_start(slot, ssem, rsem):
        for k in range(2, n_seq, 2):
            push(slot(s), slot(s), ssem.at[k], rsem.at[k], to_seq(k))
        push(slot(s), slot(s), ssem.at[1], rsem.at[1], to_seq(1))

    def gather_relay(slot, ssem, rsem):
        for k in range(2, n_seq, 2):
            arrived(slot(flip(s, k)), ssem.at[k], rsem.at[k], to_seq(k))
            push(slot(flip(s, k)), slot(flip(s, k)), ssem.at[k + 1], rsem.at[k + 1], to_seq(1))

    def gather_end(slot, ssem, rsem):
        for k in range(1, n_seq, 2):
            arrived(slot(flip(s, k)), ssem.at[k], rsem.at[k], to_seq(1))

    load = pltpu.make_async_copy(video, vid, vid_sem)
    load.start()

    def qw_slot(p):
        return qwg.at[pl.ds(pl.multiple_of(p * depth, depth), depth), :]

    own_qw = pltpu.make_async_copy(qw, qw_slot(s), loc_sem.at[0])
    own_qw.start()
    own_ctx = pltpu.make_async_copy(ctx.at[s], ctxg.at[s], loc_sem.at[1])
    own_ctx.start()
    piece = ow.shape[0] // n_seq

    def ow_piece(p):
        return pl.ds(pl.multiple_of(p * piece, piece), piece)

    own_spread = pltpu.make_async_copy(ow.at[ow_piece(s), :], spread.at[s], loc_sem.at[2])
    own_spread.start()

    barrier = pltpu.get_barrier_semaphore()
    for k in range(1, n_seq):
        pl.semaphore_signal(barrier, inc=1, device_id=to_seq(k), device_id_type=MESH_ID)
    for k in range(1, n_head):
        pl.semaphore_signal(barrier, inc=1, device_id=to_head(k), device_id_type=MESH_ID)
    pl.semaphore_wait(barrier, n_seq + n_head - 2)

    for k in range(1, n_seq):
        push(ctx.at[flip(s, k)], ctxg.at[s], ctx_s.at[k], ctx_r.at[k], to_seq(k))
    own_qw.wait()
    gather_start(qw_slot, qw_s, qw_r)
    for k in range(1, n_seq):
        push(ow.at[ow_piece(flip(s, k)), :], spread.at[s], sp_s.at[k], sp_r.at[k], to_seq(k))

    load.wait()
    strip = 16

    @pl.loop(0, tok // strip)
    def _(i):
        at = pl.ds(pl.multiple_of(i * strip, strip), strip)
        rows = vid[at, :].astype(F32)
        mean = jnp.mean(rows, axis=-1, keepdims=True)
        centred = rows - mean
        spread_ = jnp.mean(centred * centred, axis=-1, keepdims=True)
        normed[at, :] = (centred / jnp.sqrt(spread_ + 1e-06)).astype(BF16)

    own_ctx.wait()
    for k in range(1, n_seq):
        arrived(ctxg.at[flip(s, k)], ctx_s.at[k], ctx_r.at[k], to_seq(k))
    source = ctxg[...].reshape(n_seq * text, depth)
    keys = jnp.dot(source, kw[...], preferred_element_type=F32)
    part[:, :, :, :att] = keys.reshape(n_chip, 2, text, att)
    values = jnp.dot(source, vw[...], preferred_element_type=F32)
    part[:, :, :, att:] = values.reshape(n_chip, 2, text, att)
    push(part.at[:, 1 - core], pair, pr_s, pr_r, to_seq(1))

    for i in range(2):
        shsc[i] = mod[i : i + 1, :] + jnp.dot(act[...], tw[i], preferred_element_type=F32)[:8]

    arrived(pair, pr_s, pr_r, to_seq(1))
    for c in range(n_chip):
        rsg[0, c] = part[c, core] + pair[c]
    for k in range(1, n_chip):
        push(
            rsg.at[0, flip(chip, k)], rsg.at[k, chip], rs_s.at[k], rs_r.at[k], to_seq(2 * k)
        )

    own_spread.wait()
    for k in range(1, n_seq):
        arrived(spread.at[flip(s, k)], sp_s.at[k], sp_r.at[k], to_seq(k))

    def own_cols(zz):
        return pl.ds(zz * ratio, ratio)

    own_ow = pltpu.make_async_copy(
        spread.at[own_cols(z)], owg.at[:, z, ow_piece(s), :], loc_sem.at[3]
    )
    own_ow.start()
    for k in range(1, n_head):
        push(
            spread.at[own_cols(flip(z, k))], owg.at[:, z, ow_piece(s), :],
            oz_s.at[k], oz_r.at[k], to_head(k),
        )

    gather_relay(qw_slot, qw_s, qw_r)
    gather_end(qw_slot, qw_s, qw_r)
    queries[...] = jnp.dot(normed[...], qwg[...], preferred_element_type=F32)
    q_sum = jnp.sum(queries[...] * queries[...], axis=1, keepdims=True)
    qsq[0] = rows_to_lanes(q_sum, tok)

    total = rsg[0, chip]
    for k in range(1, n_chip):
        arrived(rsg.at[k, flip(chip, k)], rs_s.at[k], rs_r.at[k], to_seq(2 * k))
        total = total + rsg[k, flip(chip, k)]
    key_rows = total[:, :att]
    k_sum = jnp.sum(key_rows * key_rows, axis=1, keepdims=True)
    ksq[0] = jnp.broadcast_to(k_sum, (text, LANES))
    for k in range(1, n_head):
        push(ksq.at[0], ksq.at[k], ksq_s.at[k], ksq_r.at[k], to_head(k))
    for k in range(1, n_head):
        push(qsq.at[0], qsq.at[k], qsq_s.at[k], qsq_r.at[k], to_head(k))
    for k in range(1, n_head):
        arrived(ksq.at[k], ksq_s.at[k], ksq_r.at[k], to_head(k))
    k_mean = jnp.sum(ksq[...], axis=0)[:, :1] / (att * n_head)
    own_kv[:, :att] = (key_rows / jnp.sqrt(k_mean + 1e-06) * kg[...]).astype(BF16)
    own_kv[:, att:] = total[:, att:].astype(BF16)
    kvg[s] = own_kv[...]

    def kv_slot(p):
        return kvg.at[p]

    gather_start(kv_slot, kv_s, kv_r)

    for k in range(1, n_head):
        arrived(qsq.at[k], qsq_s.at[k], qsq_r.at[k], to_head(k))
    q_lane = jnp.sum(qsq[...], axis=0)
    q_mean = jnp.transpose(q_lane)[:, :1] / (att * n_head)
    q_normed = (queries[...] / jnp.sqrt(q_mean + 1e-06) * qg[...]).astype(BF16)

    own_ow.wait()
    for k in range(1, n_head):
        arrived(owg.at[:, flip(z, k), ow_piece(s), :], oz_s.at[k], oz_r.at[k], to_head(k))

    def ow_slot(p):
        return owg.at[:, :, ow_piece(p), :]

    gather_relay(kv_slot, kv_s, kv_r)
    gather_start(ow_slot, og_s, og_r)
    gather_end(kv_slot, kv_s, kv_r)

    every = kvg[...].reshape(n_seq * text, 2 * att)
    all_text = n_seq * text
    seen = lax.broadcasted_iota(jnp.int32, (1, all_text), 1) < valid[0]
    step = tok // chunks
    for c in range(chunks):
        at = slice(c * step, (c + 1) * step)
        for h in range(att // HD):
            lanes = slice(h * HD, (h + 1) * HD)
            scores = lax.dot_general(
                q_normed[at, lanes], every[:, lanes], (((1,), (1,)), ((), ())),
                preferred_element_type=F32,
            ) * HD ** (-0.5)
            scores = jnp.where(seen, scores, F32(-1e30))
            shifted = jnp.exp(scores - jnp.max(scores, axis=-1, keepdims=True))
            weights = (shifted / jnp.sum(shifted, axis=-1, keepdims=True)).astype(BF16)
            attg[0, at, lanes] = jnp.dot(
                weights, every[:, att + h * HD : att + (h + 1) * HD],
                preferred_element_type=F32,
            ).astype(BF16)
        for k in range(1, n_head):
            push(
                attg.at[0, at], attg.at[k, at],
                at_s.at[c, k], at_r.at[c, k], to_head(k),
            )
    gather_relay(ow_slot, og_s, og_r)
    gather_end(ow_slot, og_s, og_r)

    cols = owg.shape[3]
    sums = []
    squares = []
    for c in range(chunks):
        at = slice(c * step, (c + 1) * step)
        for k in range(1, n_head):
            arrived(attg.at[k, at], at_s.at[c, k], at_r.at[c, k], to_head(k))
        row_sum = jnp.zeros((step, 1), F32)
        row_sq = jnp.zeros((step, 1), F32)
        for j in range(ratio):
            here = slice(j * cols, (j + 1) * cols)
            projected = jnp.dot(attg[0, at], owg[j, z], preferred_element_type=F32)
            for k in range(1, n_head):
                projected = projected + jnp.dot(
                    attg[k, at], owg[j, flip(z, k)], preferred_element_type=F32
                )
            rounded = (vpart[at, here].astype(F32) + projected).astype(BF16)
            resid_out[at, here] = rounded
            wide = rounded.astype(F32)
            row_sum = row_sum + jnp.sum(wide, axis=1, keepdims=True)
            row_sq = row_sq + jnp.sum(wide * wide, axis=1, keepdims=True)
        sums.append(row_sum)
        squares.append(row_sq)
    stat[0, :8] = rows_to_lanes(jnp.concatenate(sums, axis=0), tok)
    stat[0, 8:] = rows_to_lanes(jnp.concatenate(squares, axis=0), tok)
    for k in range(1, n_head):
        push(stat.at[0], stat.at[k], st_s.at[k], st_r.at[k], to_head(k))
    for k in range(1, n_head):
        arrived(stat.at[k], st_s.at[k], st_r.at[k], to_head(k))
    both = jnp.sum(stat[...], axis=0) / (mod_out.shape[1] * n_head)
    mean2 = both[:8]
    inverse = 1.0 / jnp.sqrt(both[8:] - mean2 * mean2 + 1e-06)
    mean_col = jnp.transpose(mean2)[:, :1]
    inv_col = jnp.transpose(inverse)[:, :1]
    for c in range(chunks):
        at = slice(c * step, (c + 1) * step)
        wide = resid_out[at, :].astype(F32)
        mod_out[at, :] = (
            (wide - mean_col[at]) * inv_col[at] * (1.0 + shsc[1, :1, :]) + shsc[0, :1, :]
        ).astype(BF16)
    for copy in sent:
        copy.wait_send()


def on_device(
    n_seq,
    n_head,
    video_rows,
    context,
    valid_length,
    timestep,
    query_weight,
    key_weight,
    value_weight,
    out_weight,
    query_gain,
    key_gain,
    time_weight,
    modulation,
):
    tok, width = video_rows.shape
    text = context.shape[0]
    depth, att = query_weight.shape
    cols = out_weight.shape[1]
    part_width = modulation.shape[1]
    ratio = n_seq // n_head
    n_chip = n_seq // 2
    chunks = 4
    piece = out_weight.shape[0] // n_seq
    half = FREQ // 2
    freqs = jnp.exp(-jnp.log(10000.0) * jnp.arange(half, dtype=F32) / half)
    angles = timestep[0].astype(F32) * freqs
    embedding = jnp.concatenate([jnp.cos(angles), jnp.sin(angles)])
    act = jnp.broadcast_to(jax.nn.silu(embedding).astype(BF16)[None, :], (16, FREQ))
    blocks = context.reshape(text, n_seq, depth).transpose(1, 0, 2)
    vpart = lax.dynamic_slice_in_dim(
        video_rows, lax.axis_index("head") * part_width, part_width, 1
    )
    vmem = pl.BlockSpec(memory_space=pltpu.VMEM)
    dma = pltpu.SemaphoreType.DMA
    seq_sems = [dma((n_seq,))] * 2
    head_sems = [dma((n_head,))] * 2
    return pl.pallas_call(
        functools.partial(body, n_seq, n_head, chunks),
        out_shape=[jax.ShapeDtypeStruct((tok, part_width), BF16)] * 2,
        in_specs=[
            pl.BlockSpec(memory_space=pltpu.SMEM),
            pl.BlockSpec(memory_space=pl.ANY),
        ]
        + [vmem] * 11,
        out_specs=[vmem] * 2,
        scratch_shapes=[
            pltpu.VMEM((tok, width), BF16),
            pltpu.VMEM((tok, width), BF16),
            pltpu.VMEM((n_seq, text, depth), BF16),
            pltpu.VMEM((n_seq * depth, att), BF16),
            pltpu.VMEM((n_chip, 2, text, 2 * att), F32),
            pltpu.VMEM((n_chip, text, 2 * att), F32),
            pltpu.VMEM((n_chip, n_chip, text, 2 * att), F32),
            pltpu.VMEM((text, 2 * att), BF16),
            pltpu.VMEM((n_seq, text, 2 * att), BF16),
            pltpu.VMEM((n_seq, piece, cols), BF16),
            pltpu.VMEM((ratio, n_head, out_weight.shape[0], cols), BF16),
            pltpu.VMEM((n_head, tok, att), BF16),
            pltpu.VMEM((tok, att), F32),
            pltpu.VMEM((n_head, 8, tok), F32),
            pltpu.VMEM((n_head, text, LANES), F32),
            pltpu.VMEM((n_head, 16, tok), F32),
            pltpu.VMEM((2, 8, part_width), F32),
            dma,
            dma((4,)),
            *seq_sems,
            *seq_sems,
            dma,
            dma,
            *[dma((n_chip,))] * 2,
            *seq_sems,
            *seq_sems,
            *head_sems,
            *seq_sems,
            *head_sems,
            *head_sems,
            *[dma((chunks, n_head))] * 2,
            *head_sems,
        ],
        compiler_params=pltpu.CompilerParams(
            collective_id=0, has_side_effects=True, vmem_limit_bytes=60 * 1024 * 1024
        ),
    )(
        valid_length,
        video_rows,
        blocks,
        query_weight,
        key_weight,
        value_weight,
        out_weight,
        query_gain[None, :],
        key_gain[None, :],
        act,
        time_weight,
        modulation,
        vpart,
    )


def solution(mesh):
    in_specs = (
        P("seq", None),
        P("seq", None),
        P(),
        P(),
        P("seq", "head"),
        P("seq", "head"),
        P("seq", "head"),
        P("head", "seq"),
        P("head"),
        P("head"),
        P(None, None, "head"),
        P(None, "head"),
    )
    out_specs = (P("seq", "head"), P("seq", "head"))
    return jax.shard_map(
        functools.partial(on_device, mesh.shape["seq"], mesh.shape["head"]),
        mesh=mesh, in_specs=in_specs, out_specs=out_specs, check_vma=False,
    )
```
